32 devices in a mesh: video: 8 (over y, x, core), head: 4 (over z).
Axes of the slice: x: 2, y: 2, z: 4, core: 2. Of those that a mesh axis runs over, the one named last changes fastest.
Arguments:
- text_queries: bfloat16 [128, 8192], P('video', 'head'), may hold values from -140 to 140
- visual_keys: bfloat16 [4096, 1024], P('video', 'head'), may hold values from -5 to 5
- visual_values: bfloat16 [4096, 1024], P('video', 'head'), may hold values from -6 to 6
- out_grad: bfloat16 [128, 8192], P('video', 'head'), may hold values from -384 to 384
- query_frame: int32 [128], replicated, may hold values from 0 to 15
- block_frame: int32 [32], replicated, may hold values from 0 to 16, as said below
- q_weight: bfloat16 [8192, 8192], P('head', 'video'), may hold values from -0.0625 to 0.0625
Outputs:
- query_grad: bfloat16 [128, 8192], P('video', 'head')
- key_grad: bfloat16 [4096, 1024], P('video', 'head')
- value_grad: bfloat16 [4096, 1024], P('video', 'head')
- text_grad: bfloat16 [128, 8192], P('head', 'video')
The draws below stay inside these ranges and needn't reach their ends.
Inputs may be any that keep to these rules, and one draw needn't show every extreme that they name: `block_frame`: on each index of video the first 1 to 4 block slots are live and the rest empty; some index has all 4 live. Live blocks carry frame numbers that never fall along the whole array and start at 0; empty slots carry 16.
All inputs are finite; a program needn't handle non-finite values.
Results may differ from the reference program's by a relative error of at most 0.0058.
Values may be sent and summed in bfloat16 or wider, within the bound.
A program may use at most 384 MiB of HBM per device.

```python
import jax
import jax.numpy as jnp
from jax import lax

D = 8192
HEADS = 64
KV_HEADS = 8
HEAD_DIM = 128
BLK_DEV = 4
BLOCK = 128
FRAMES = 16
QUERIES = 128
NBLK = 32
NKEYS = 4096


def keys_source(key):
    source = jax.random.normal(jax.random.fold_in(key, 11), (NKEYS, KV_HEADS * HEAD_DIM), jnp.float32)
    source = jnp.clip(source, -5.0, 5.0)
    return source.at[1].set(source[0] * 0.992)


def draw_visual_keys(key, part):
    return keys_source(key).astype(jnp.bfloat16)


def draw_text_queries(key, part):
    drawn = jax.random.normal(jax.random.fold_in(key, 12), (QUERIES, HEADS * HEAD_DIM), jnp.float32)
    drawn = jnp.clip(drawn, -5.0, 5.0)
    return drawn.astype(jnp.bfloat16)


def draw_block_frame(key, part):
    devices = NBLK // BLK_DEV
    counts = jax.random.randint(jax.random.fold_in(key, 21), (devices,), 1, BLK_DEV + 1)
    fullest = jax.random.randint(jax.random.fold_in(key, 22), (), 0, devices)
    counts = jnp.where(jnp.arange(devices) == fullest, BLK_DEV, counts)
    slot_index = jnp.arange(NBLK) % BLK_DEV
    live_slots = (slot_index < jnp.repeat(counts, BLK_DEV)).astype(jnp.int32)
    ranking = jnp.cumsum(live_slots) - 1
    live_total = jnp.sum(live_slots)
    return jnp.where(live_slots > 0, ranking * FRAMES // live_total, FRAMES).astype(jnp.int32)


def set_ends(drawn, stream_key, low, high):
    longest = drawn.shape.index(max(drawn.shape))
    spots = []
    for shift in (0, 1):
        where = [jax.random.randint(jax.random.fold_in(stream_key, axis), (), 0, length) for axis, length in enumerate(drawn.shape)]
        where[longest] = (where[longest] + shift) % drawn.shape[longest]
        spots.append(tuple(where))
    return drawn.at[spots[0]].set(low).at[spots[1]].set(high)


def level_of(stream_key, extent, split, smallest, high):
    gain, own = 1.0, jax.random.fold_in(stream_key, 6)
    for dim, parts in split:
        steps = jnp.exp(jax.random.uniform(jax.random.fold_in(own, dim), (parts,), jnp.float32, smallest / len(split), high / len(split)))
        gain = gain * jnp.repeat(steps, extent[dim] // parts).reshape([-1 if axis == dim else 1 for axis in range(len(extent))])
    return gain


def bell_draw(stream_key, shape, width, most, cuts=(), kind=jnp.bfloat16):
    values = jax.random.normal(stream_key, shape, jnp.float32) * width
    if len(cuts) > 0:
        values = level_of(stream_key, shape, cuts, -0.22, 0.18) * values
    return jnp.clip(values, min=-most, max=most).astype(kind)


def setup_inputs(seed: int = 0) -> dict:
    key_list = jax.random.split(jax.random.key(seed), 8)
    return {
        "text_queries": draw_text_queries(jax.random.fold_in(key_list[7], 71), 0),
        "visual_keys": draw_visual_keys(jax.random.fold_in(key_list[7], 71), 0),
        "visual_values": bell_draw(key_list[2], (NKEYS, KV_HEADS * HEAD_DIM), 1.0, 6.0, ((0, 8), (1, 4))),
        "out_grad": bell_draw(key_list[3], (QUERIES, HEADS * HEAD_DIM), (NKEYS // 64), 384.0, ((0, 8), (1, 4))),
        "query_frame": set_ends(jax.random.randint(key_list[4], (QUERIES,), 0, FRAMES), jax.random.fold_in(key_list[4], 1), 0, FRAMES - 1).astype(jnp.int32),
        "block_frame": draw_block_frame(jax.random.fold_in(key_list[7], 71), 0),
        "q_weight": bell_draw(key_list[6], (HEADS * HEAD_DIM, D), (HEADS * HEAD_DIM) ** -0.5, 0.0625, ((0, 4), (1, 8))),
    }


neg_fill = -1.0e30


def reference(text_queries, visual_keys, visual_values, out_grad, query_frame, block_frame, q_weight):
    group_size = HEADS // KV_HEADS
    score_scale = HEAD_DIM ** -0.5
    highest = lax.Precision.HIGHEST
    query_heads = text_queries.astype(jnp.float32).reshape(QUERIES, KV_HEADS, group_size, HEAD_DIM)
    grad_heads = out_grad.astype(jnp.float32).reshape(QUERIES, KV_HEADS, group_size, HEAD_DIM)
    key_blocks = visual_keys.astype(jnp.float32).reshape(NBLK, BLOCK, KV_HEADS, HEAD_DIM)
    value_blocks = visual_values.astype(jnp.float32).reshape(NBLK, BLOCK, KV_HEADS, HEAD_DIM)

    def masked(key_block, frame):
        scores = jnp.einsum("rgjd,kgd->rgjk", query_heads, key_block, precision=highest) * score_scale
        visible = (frame <= query_frame)[:, None, None, None]
        return jnp.where(visible, scores, neg_fill), visible

    def forward(running, block_items):
        peaks, totals, weighted = running
        key_block, value_block, frame = block_items
        scores, visible = masked(key_block, frame)
        new_peak = jnp.maximum(peaks, jnp.max(scores, axis=-1))
        rescale = jnp.exp(peaks - new_peak)
        weights = jnp.where(visible, jnp.exp(scores - new_peak[..., None]), 0.0)
        totals = totals * rescale + jnp.sum(weights, axis=-1)
        weighted = weighted * rescale[..., None] + jnp.einsum("rgjk,kgd->rgjd", weights, value_block, precision=highest)
        return (new_peak, totals, weighted), None

    start_state = (jnp.full((QUERIES, KV_HEADS, group_size), neg_fill, jnp.float32),
                   jnp.zeros((QUERIES, KV_HEADS, group_size), jnp.float32),
                   jnp.zeros((QUERIES, KV_HEADS, group_size, HEAD_DIM), jnp.float32))
    final_state, unused = lax.scan(forward, start_state, (key_blocks, value_blocks, block_frame))
    peaks, totals, weighted = final_state
    log_total = peaks + jnp.log(totals)
    row_dots = jnp.sum(grad_heads * (weighted / totals[..., None]), axis=-1)

    def backward(query_sum, block_items):
        key_block, value_block, frame = block_items
        scores, visible = masked(key_block, frame)
        weights = jnp.where(visible, jnp.exp(scores - log_total[..., None]), 0.0)
        value_dots = jnp.einsum("rgjd,kgd->rgjk", grad_heads, value_block, precision=highest)
        grads_half = lax.optimization_barrier((weights * (value_dots - row_dots[..., None])).astype(jnp.bfloat16))
        weight_half = lax.optimization_barrier(weights.astype(jnp.bfloat16))
        score_grads = grads_half.astype(jnp.float32)
        weight_back = weight_half.astype(jnp.float32)
        query_sum = query_sum + jnp.einsum("rgjk,kgd->rgjd", score_grads, key_block, precision=highest) * score_scale
        key_part = jnp.einsum("rgjk,rgjd->kgd", score_grads, query_heads, precision=highest) * score_scale
        value_part = jnp.einsum("rgjk,rgjd->kgd", weight_back, grad_heads, precision=highest)
        return query_sum, (key_part.astype(jnp.bfloat16), value_part.astype(jnp.bfloat16))

    query_start = jnp.zeros((QUERIES, KV_HEADS, group_size, HEAD_DIM), jnp.float32)
    query_sum, key_value = lax.scan(backward, query_start, (key_blocks, value_blocks, block_frame))
    query_grad = query_sum.reshape(QUERIES, HEADS * HEAD_DIM).astype(jnp.bfloat16)
    key_grad = key_value[0].reshape(NKEYS, KV_HEADS * HEAD_DIM)
    value_grad = key_value[1].reshape(NKEYS, KV_HEADS * HEAD_DIM)
    text_grad = jnp.dot(query_grad, q_weight, preferred_element_type=jnp.float32).astype(jnp.bfloat16)
    return (query_grad, key_grad, value_grad, text_grad)
```

```python
import functools

import jax
import jax.numpy as jnp
from jax import lax
from jax.experimental import pallas as pl
from jax.experimental.pallas import tpu as pltpu
from jax.sharding import PartitionSpec as P

HEADS = 64
KV_HEADS = 8
HEAD_DIM = 128
BLOCK = 128
GROUP = HEADS // KV_HEADS
CH = 4
FAR = -1.0e30
SCALE = HEAD_DIM ** (-0.5)
NT = (((1,), (1,)), ((), ()))
F32 = jnp.float32
BF16 = jnp.bfloat16


def kernel(
    V, H, qf_ref, bf_ref, q_ref, do_ref, k_ref, v_ref, w_ref,
    qg_out, kg_out, vg_out, tg_out,
    land, keys, vals, keysT, wts, bias, probs, dots, peaks, stats, coef, dqp, dqs, own, rsb, rsl,
    qg, acc, tb, tl, tout, kacc, vacc, kout, vout,
    load_sem, own_sem, out_sem, qout_sem,
    g_send, g_recv, f_send, f_recv, st_send, st_recv, x_send, x_recv, r_send, r_recv,
    a_send, a_recv, b_send, b_recv, z_send, z_recv,
):
    C = V // 2
    me = lax.axis_index("video")
    z = lax.axis_index("head")
    c = me // 2
    core = lax.rem(me, 2)
    mate = c * 2 + (1 - core)
    K = land.shape[0]
    R = q_ref.shape[0]
    NQ = V * R
    T = k_ref.shape[0]
    NB = T // BLOCK
    G = k_ref.shape[1] // HEAD_DIM
    CW = CH * HEAD_DIM
    NW = w_ref.shape[1]
    CZ = C // H
    ins = (q_ref, do_ref)

    def local(src, dst, sem):
        return pltpu.make_async_copy(src, dst, sem)

    def remote(src, dst, ssem, rsem, axis, target):
        pltpu.make_async_remote_copy(
            src_ref=src, dst_ref=dst, send_sem=ssem, recv_sem=rsem,
            device_id={axis: target}, device_id_type=pl.DeviceIdType.MESH,
        ).start()

    def wait(ref, sem):
        pltpu.make_async_copy(ref, ref, sem).wait()

    for k in range(K):
        for a in range(2):
            local(ins[a].at[:, pl.ds(k * CW, CW)], land.at[k, a, core, c], own_sem.at[k, a]).start()
    local(k_ref, keys, load_sem.at[0]).start()
    local(v_ref, vals, load_sem.at[1]).start()
    local(w_ref, wts, load_sem.at[2]).start()

    barrier = pltpu.get_barrier_semaphore()
    for o in range(1, V):
        pl.semaphore_signal(
            barrier, inc=1, device_id={"video": lax.rem(me + o, V)},
            device_id_type=pl.DeviceIdType.MESH,
        )
    for o in range(1, H):
        pl.semaphore_signal(
            barrier, inc=1, device_id={"head": lax.rem(z + o, H)},
            device_id_type=pl.DeviceIdType.MESH,
        )
    pl.semaphore_wait(barrier, V - 1 + H - 1)

    chips = [lax.rem(c + o, C) for o in range(1, C)]

    for k in range(K):
        for a in range(2):
            for cc in chips:
                remote(
                    ins[a].at[:, pl.ds(k * CW, CW)], land.at[k, a, core, c],
                    g_send.at[k, a], g_recv.at[k, a], "video", cc * 2 + core,
                )

    for b in range(NB):
        seen = bf_ref[me * NB + b] <= qf_ref[...]
        bias[pl.ds(b, 1), :] = jnp.where(seen, 0.0, FAR).astype(F32)
    wait(keys, load_sem.at[0])
    for g in range(G):
        part = keys[:, g * HEAD_DIM:(g + 1) * HEAD_DIM].astype(F32)
        keysT[g] = part.T.astype(BF16)
    wait(vals, load_sem.at[1])

    def arrive(k):
        for a in range(2):
            wait(land.at[k, a, core, c], own_sem.at[k, a])
            wait(land.at[k, a, core, pl.ds(0, C - 1)], g_recv.at[k, a])
            remote(
                land.at[k, a, core], land.at[k, a, core],
                f_send.at[k, a], f_recv.at[k, a], "video", mate,
            )

    def heads_of(k, a, hh):
        cols = pl.ds(pl.multiple_of(hh * HEAD_DIM, HEAD_DIM), HEAD_DIM)
        return land[k, a, :, :, :, cols].reshape(NQ, HEAD_DIM)

    def group_of(k):
        return (k * CH) // GROUP

    def forward(k):
        for a in range(2):
            wait(land.at[k, a, 1 - core], f_recv.at[k, a])
        g = group_of(k)
        feats = slice(g * HEAD_DIM, (g + 1) * HEAD_DIM)

        def head(hh, carry):
            s = lax.dot_general(keys[:, feats], heads_of(k, 0, hh), NT, preferred_element_type=F32)
            s = s.reshape(NB, BLOCK, NQ) * SCALE + bias[...].reshape(NB, 1, NQ)
            s = s.reshape(T, NQ)
            m = jnp.max(s, axis=0, keepdims=True)
            m = jnp.where(m > 0.1 * FAR, m, 0.0)
            p = jnp.exp(s - m)
            total = jnp.sum(p, axis=0, keepdims=True)
            d = lax.dot_general(vals[:, feats], heads_of(k, 1, hh), NT, preferred_element_type=F32)
            r = jnp.sum(p * d, axis=0, keepdims=True)
            probs[k * CH + hh] = p
            dots[k * CH + hh] = d
            live = total > 0.0
            safe = jnp.where(live, total, 1.0)
            peaks[k, pl.ds(hh, 1), :] = m
            stats[k, me, pl.ds(hh, 1), :] = jnp.where(live, m + jnp.log(safe), FAR)
            stats[k, me, pl.ds(CH + hh, 1), :] = r / safe
            return carry

        lax.fori_loop(0, CH, head, 0)
        for o in range(1, V):
            remote(
                stats.at[k, me], stats.at[k, me], st_send.at[k], st_recv.at[k],
                "video", lax.rem(me + o, V),
            )

    def weights_of(k, hh):
        w = probs[k * CH + hh] * coef[k, pl.ds(hh, 1), :]
        ds = w * (dots[k * CH + hh] - coef[k, pl.ds(CH + hh, 1), :])
        return w, ds.astype(BF16)

    def backward(k):
        wait(stats.at[k, pl.ds(0, V - 1)], st_recv.at[k])
        parts = stats[k]
        logs, rows = parts[:, :CH], parts[:, CH:]
        top = jnp.max(logs, axis=0)
        e = jnp.exp(logs - top[None])
        total = jnp.sum(e, axis=0)
        log_total = top + jnp.log(total)
        coef[k, pl.ds(0, CH), :] = jnp.exp(jnp.minimum(peaks[k] - log_total, 0.0))
        coef[k, pl.ds(CH, CH), :] = jnp.sum(e * rows, axis=0) / total
        g = group_of(k)

        def head(hh, carry):
            w, ds = weights_of(k, hh)
            dqT = jnp.dot(keysT[g], ds, preferred_element_type=F32)
            cols = pl.ds(pl.multiple_of(hh * HEAD_DIM, HEAD_DIM), HEAD_DIM)
            dqp[k, :, :, :, cols] = dqT.T.reshape(2, C, R, HEAD_DIM)
            return carry

        lax.fori_loop(0, CH, head, 0)
        remote(dqp.at[k, 1 - core], dqs.at[k], x_send.at[k], x_recv.at[k], "video", mate)

    def pair_sum(k):
        wait(dqs.at[k], x_recv.at[k])
        s = dqp[k, core] + dqs[k]
        own[k] = s
        rsb[k] = s.astype(BF16)
        for cc in chips:
            remote(
                rsb.at[k, cc], rsl.at[k, c], r_send.at[k], r_recv.at[k], "video", cc * 2 + core
            )

    def total_sum(k):
        wait(rsl.at[k, pl.ds(0, C - 1)], r_recv.at[k])
        s = own[k, c]
        for cc in chips:
            s = s + rsl[k, cc].astype(F32)
        qg[k, core, c] = (s * SCALE).astype(BF16)
        for cc in chips:
            remote(
                qg.at[k, core, c], qg.at[k, core, c], a_send.at[k], a_recv.at[k],
                "video", cc * 2 + core,
            )
        local(qg.at[k, core, c], qg_out.at[:, pl.ds(k * CW, CW)], qout_sem.at[k]).start()

    def spread(k):
        wait(qg.at[k, core, pl.ds(0, C - 1)], a_recv.at[k])
        remote(qg.at[k, core], qg.at[k, core], b_send.at[k], b_recv.at[k], "video", mate)

    def text(k):
        wait(qg.at[k, 1 - core], b_recv.at[k])
        if k == 0:
            wait(wts, load_sem.at[2])
        x = qg[k].reshape(NQ, CW)
        part = jnp.dot(x, wts[k * CW:(k + 1) * CW, :], preferred_element_type=F32)
        part = part.reshape(2, C, R, NW)
        if k > 0:
            part = part + acc[...]
        if k < K - 1:
            acc[...] = part
        else:
            acc[...] = part
            tb[...] = part.astype(BF16)

    def key_value(k):
        g = group_of(k)
        fresh = (k * CH) % GROUP == 0
        last = ((k + 1) * CH) % GROUP == 0
        if fresh:
            kacc[...] = jnp.zeros_like(kacc)
            vacc[...] = jnp.zeros_like(vacc)

        def head(hh, carry):
            w, ds = weights_of(k, hh)
            kacc[...] += jnp.dot(ds, heads_of(k, 0, hh), preferred_element_type=F32)
            vacc[...] += jnp.dot(w.astype(BF16), heads_of(k, 1, hh), preferred_element_type=F32)
            return carry

        lax.fori_loop(0, CH, head, 0)
        if last:
            feats = pl.ds(g * HEAD_DIM, HEAD_DIM)
            kout[g] = (kacc[...] * SCALE).astype(BF16)
            vout[g] = vacc[...].astype(BF16)
            local(kout.at[g], kg_out.at[:, feats], out_sem.at[0, g]).start()
            local(vout.at[g], vg_out.at[:, feats], out_sem.at[1, g]).start()

    for k in range(K):
        arrive(k)
        if k:
            forward(k - 1)
    forward(K - 1)
    for k in range(K):
        backward(k)
        if k:
            pair_sum(k - 1)
    pair_sum(K - 1)
    for k in range(K):
        total_sum(k)
        if k < K - 2:
            key_value(k)
    for k in range(K):
        spread(k)
        if k:
            text(k - 1)
    text(K - 1)
    for o in range(1, H):
        zz = lax.rem(z + o, H)
        remote(tb.at[:, pl.ds(zz * CZ, CZ)], tl.at[z], z_send, z_recv, "head", zz)
    for k in range(max(K - 2, 0), K):
        key_value(k)
    wait(tl.at[pl.ds(0, H - 1)], z_recv)
    for i in range(CZ):
        for half in range(2):
            s = acc[half, z * CZ + i]
            for o in range(1, H):
                s = s + tl[lax.rem(z + o, H), half, i].astype(F32)
            tout[pl.ds((i * 2 + half) * R, R), :] = s.astype(BF16)
    local(tout, tg_out, load_sem.at[0]).start()

    for k in range(K):
        for a in range(2):
            wait(land.at[k, a, core, pl.ds(0, C - 1)], g_send.at[k, a])
            wait(land.at[k, a, core], f_send.at[k, a])
        wait(stats.at[k, pl.ds(0, V - 1)], st_send.at[k])
        wait(dqs.at[k], x_send.at[k])
        wait(rsl.at[k, pl.ds(0, C - 1)], r_send.at[k])
        wait(qg.at[k, core, pl.ds(0, C - 1)], a_send.at[k])
        wait(qg.at[k, core], b_send.at[k])
        wait(qg.at[k, core, c], qout_sem.at[k])
    wait(tl.at[pl.ds(0, H - 1)], z_send)
    for g in range(G):
        wait(kout.at[g], out_sem.at[0, g])
        wait(vout.at[g], out_sem.at[1, g])
    wait(tout, load_sem.at[0])


def shards(V, H, text_queries, visual_keys, visual_values, out_grad, query_frame, block_frame, q_weight):
    R, QW = text_queries.shape
    T, KW = visual_keys.shape
    C = V // 2
    NQ = V * R
    NW = q_weight.shape[1]
    HL = QW // HEAD_DIM
    G = KW // HEAD_DIM
    K = HL // CH
    CW = CH * HEAD_DIM
    CZ = C // H
    frames = query_frame.reshape(C, 2, R).transpose(1, 0, 2).reshape(1, NQ)
    vmem = pltpu.VMEM
    dma = pltpu.SemaphoreType.DMA
    any_spec = pl.BlockSpec(memory_space=pl.ANY)
    return pl.pallas_call(
        functools.partial(kernel, V, H),
        out_shape=(
            jax.ShapeDtypeStruct((R, QW), BF16),
            jax.ShapeDtypeStruct((T, KW), BF16),
            jax.ShapeDtypeStruct((T, KW), BF16),
            jax.ShapeDtypeStruct((NQ // H, NW), BF16),
        ),
        in_specs=[
            pl.BlockSpec(memory_space=pltpu.VMEM),
            pl.BlockSpec(memory_space=pltpu.SMEM),
        ] + [any_spec] * 5,
        out_specs=(any_spec,) * 4,
        scratch_shapes=[
            vmem((K, 2, 2, C, R, CW), BF16),
            vmem((T, KW), BF16),
            vmem((T, KW), BF16),
            vmem((G, HEAD_DIM, T), BF16),
            vmem((QW, NW), BF16),
            vmem((T // BLOCK, NQ), F32),
            vmem((HL, T, NQ), F32),
            vmem((HL, T, NQ), F32),
            vmem((K, CH, NQ), F32),
            vmem((K, V, 2 * CH, NQ), F32),
            vmem((K, 2 * CH, NQ), F32),
            vmem((K, 2, C, R, CW), F32),
            vmem((K, C, R, CW), F32),
            vmem((K, C, R, CW), F32),
            vmem((K, C, R, CW), BF16),
            vmem((K, C, R, CW), BF16),
            vmem((K, 2, C, R, CW), BF16),
            vmem((2, C, R, NW), F32),
            vmem((2, C, R, NW), BF16),
            vmem((H, 2, CZ, R, NW), BF16),
            vmem((NQ // H, NW), BF16),
            vmem((T, HEAD_DIM), F32),
            vmem((T, HEAD_DIM), F32),
            vmem((G, T, HEAD_DIM), BF16),
            vmem((G, T, HEAD_DIM), BF16),
            dma((3,)), dma((K, 2)), dma((2, G)), dma((K,)),
            dma((K, 2)), dma((K, 2)), dma((K, 2)), dma((K, 2)),
            dma((K,)), dma((K,)), dma((K,)), dma((K,)), dma((K,)), dma((K,)),
            dma((K,)), dma((K,)), dma((K,)), dma((K,)), dma, dma,
        ],
        compiler_params=pltpu.CompilerParams(
            collective_id=0, has_side_effects=True, vmem_limit_bytes=66_000_000
        ),
    )(frames, block_frame, text_queries, out_grad, visual_keys, visual_values, q_weight)


def solution(mesh):
    in_specs = (
        P("video", "head"),
        P("video", "head"),
        P("video", "head"),
        P("video", "head"),
        P(),
        P(),
        P("head", "video"),
    )
    out_specs = (P("video", "head"), P("video", "head"), P("video", "head"), P("head", "video"))
    body = functools.partial(shards, mesh.shape["video"], mesh.shape["head"])
    return jax.shard_map(body, mesh=mesh, in_specs=in_specs, out_specs=out_specs, check_vma=False)
```

```python
import functools

import jax
import jax.numpy as jnp
from jax import lax
from jax.experimental import pallas as pl
from jax.experimental.pallas import tpu as pltpu
from jax.sharding import PartitionSpec as P

HEADS = 64
KV_HEADS = 8
HEAD_DIM = 128
BLOCK = 128
GROUP = HEADS // KV_HEADS
CH = 4
LAGS = (1, 4, 5, 8, 11, 12)
FAR = -1.0e30
SCALE = HEAD_DIM ** (-0.5)
NT = (((1,), (1,)), ((), ()))
F32 = jnp.float32
BF16 = jnp.bfloat16


def kernel(
    V, H, qf_ref, bf_ref, q_ref, do_ref, k_ref, v_ref, w_ref,
    qg_out, kg_out, vg_out, tg_out,
    land, keys, vals, keysT, wts, bias, probs, dots, peaks, stats, coef, dqp, dqs, own, rsb, rsl,
    qg, acc, tb, tl, kacc, vacc,
    load_sem, own_sem,
    g_send, g_recv, f_send, f_recv, st_send, st_recv, x_send, x_recv, r_send, r_recv,
    a_send, a_recv, b_send, b_recv, z_send, z_recv,
):
    C = V // 2
    me = lax.axis_index("video")
    z = lax.axis_index("head")
    c = me // 2
    core = lax.rem(me, 2)
    mate = c * 2 + (1 - core)
    K = land.shape[0]
    R = q_ref.shape[0]
    NQ = V * R
    T = k_ref.shape[0]
    NB = T // BLOCK
    G = k_ref.shape[1] // HEAD_DIM
    CW = CH * HEAD_DIM
    NW = w_ref.shape[1]
    CZ = C // H
    ins = (q_ref, do_ref)

    def local(src, dst, sem):
        return pltpu.make_async_copy(src, dst, sem)

    def remote(src, dst, ssem, rsem, axis, target):
        pltpu.make_async_remote_copy(
            src_ref=src, dst_ref=dst, send_sem=ssem, recv_sem=rsem,
            device_id={axis: target}, device_id_type=pl.DeviceIdType.MESH,
        ).start()

    def wait(ref, sem):
        pltpu.make_async_copy(ref, ref, sem).wait()

    for k in range(K):
        for a in range(2):
            local(ins[a].at[:, pl.ds(k * CW, CW)], land.at[k, a, core, c], own_sem.at[k, a]).start()
    local(k_ref, keys, load_sem.at[0]).start()
    local(v_ref, vals, load_sem.at[1]).start()
    local(w_ref, wts, load_sem.at[2]).start()

    barrier = pltpu.get_barrier_semaphore()
    for o in range(1, V):
        pl.semaphore_signal(
            barrier, inc=1, device_id={"video": lax.rem(me + o, V)},
            device_id_type=pl.DeviceIdType.MESH,
        )
    for o in range(1, H):
        pl.semaphore_signal(
            barrier, inc=1, device_id={"head": lax.rem(z + o, H)},
            device_id_type=pl.DeviceIdType.MESH,
        )
    pl.semaphore_wait(barrier, V - 1 + H - 1)

    chips = [lax.rem(c + o, C) for o in range(1, C)]

    for k in range(K):
        for a in range(2):
            wait(land.at[k, a, core, c], own_sem.at[k, a])
            for cc in chips:
                remote(
                    land.at[k, a, core, c], land.at[k, a, core, c],
                    g_send.at[k, a], g_recv.at[k, a], "video", cc * 2 + core,
                )

    rows = [qf_ref[:, (i * 2 + half) * R:(i * 2 + half + 1) * R] for half in range(2) for i in range(C)]
    limits = jnp.concatenate(rows, axis=1)
    for b in range(NB):
        seen = bf_ref[me * NB + b] <= limits
        bias[pl.ds(b, 1), :] = jnp.where(seen, 0.0, FAR).astype(F32)
    wait(keys, load_sem.at[0])
    for g in range(G):
        part = keys[:, g * HEAD_DIM:(g + 1) * HEAD_DIM].astype(F32)
        keysT[g] = part.T.astype(BF16)
    wait(vals, load_sem.at[1])

    def arrive(k):
        for a in range(2):
            wait(land.at[k, a, core, pl.ds(0, C - 1)], g_recv.at[k, a])
            remote(
                land.at[k, a, core], land.at[k, a, core],
                f_send.at[k, a], f_recv.at[k, a], "video", mate,
            )

    def heads_of(k, a, hh):
        cols = pl.ds(pl.multiple_of(hh * HEAD_DIM, HEAD_DIM), HEAD_DIM)
        return land[k, a, :, :, :, cols].reshape(NQ, HEAD_DIM)

    def group_of(k):
        return (k * CH) // GROUP

    def forward(k):
        for a in range(2):
            wait(land.at[k, a, 1 - core], f_recv.at[k, a])
        g = group_of(k)
        feats = slice(g * HEAD_DIM, (g + 1) * HEAD_DIM)

        def head(hh, carry):
            s = lax.dot_general(keys[:, feats], heads_of(k, 0, hh), NT, preferred_element_type=F32)
            s = s.reshape(NB, BLOCK, NQ) * SCALE + bias[...].reshape(NB, 1, NQ)
            s = s.reshape(T, NQ)
            m = jnp.max(s, axis=0, keepdims=True)
            m = jnp.where(m > 0.1 * FAR, m, 0.0)
            p = jnp.exp(s - m)
            total = jnp.sum(p, axis=0, keepdims=True)
            d = lax.dot_general(vals[:, feats], heads_of(k, 1, hh), NT, preferred_element_type=F32)
            r = jnp.sum(p * d, axis=0, keepdims=True)
            probs[k * CH + hh] = p
            dots[k * CH + hh] = d
            live = total > 0.0
            safe = jnp.where(live, total, 1.0)
            peaks[k, pl.ds(hh, 1), :] = m
            stats[k, me, pl.ds(hh, 1), :] = jnp.where(live, m + jnp.log(safe), FAR)
            stats[k, me, pl.ds(CH + hh, 1), :] = r / safe
            return carry

        lax.fori_loop(0, CH, head, 0, unroll=True)
        for o in range(1, V):
            remote(
                stats.at[k, me], stats.at[k, me], st_send.at[k], st_recv.at[k],
                "video", lax.rem(me + o, V),
            )

    def weights_of(k, hh):
        w = probs[k * CH + hh] * coef[k, pl.ds(hh, 1), :]
        ds = w * (dots[k * CH + hh] - coef[k, pl.ds(CH + hh, 1), :])
        return w, ds.astype(BF16)

    def backward(k):
        wait(stats.at[k, pl.ds(0, V - 1)], st_recv.at[k])
        parts = stats[k]
        logs, rows = parts[:, :CH], parts[:, CH:]
        top = jnp.max(logs, axis=0)
        e = jnp.exp(logs - top[None])
        total = jnp.sum(e, axis=0)
        log_total = top + jnp.log(total)
        coef[k, pl.ds(0, CH), :] = jnp.exp(jnp.minimum(peaks[k] - log_total, 0.0))
        coef[k, pl.ds(CH, CH), :] = jnp.sum(e * rows, axis=0) / total
        g = group_of(k)

        def head(hh, carry):
            w, ds = weights_of(k, hh)
            dqT = jnp.dot(keysT[g], ds, preferred_element_type=F32)
            cols = pl.ds(pl.multiple_of(hh * HEAD_DIM, HEAD_DIM), HEAD_DIM)
            dqp[k, :, :, :, cols] = dqT.T.reshape(2, C, R, HEAD_DIM)
            return carry

        lax.fori_loop(0, CH, head, 0, unroll=True)
        remote(dqp.at[k, 1 - core], dqs.at[k], x_send.at[k], x_recv.at[k], "video", mate)

    def pair_sum(k):
        wait(dqs.at[k], x_recv.at[k])
        s = dqp[k, core] + dqs[k]
        own[k] = s
        rsb[k] = s.astype(BF16)
        for cc in chips:
            remote(
                rsb.at[k, cc], rsl.at[k, c], r_send.at[k], r_recv.at[k], "video", cc * 2 + core
            )

    def total_sum(k):
        wait(rsl.at[k, pl.ds(0, C - 1)], r_recv.at[k])
        s = own[k, c]
        for cc in chips:
            s = s + rsl[k, cc].astype(F32)
        s = (s * SCALE).astype(BF16)
        qg[k, core, c] = s
        qg_out[:, k * CW:(k + 1) * CW] = s
        for cc in chips:
            remote(
                qg.at[k, core, c], qg.at[k, core, c], a_send.at[k], a_recv.at[k],
                "video", cc * 2 + core,
            )

    def spread(k):
        wait(qg.at[k, core, pl.ds(0, C - 1)], a_recv.at[k])
        remote(qg.at[k, core], qg.at[k, core], b_send.at[k], b_recv.at[k], "video", mate)

    def product(k, half, phase):
        x = qg[k, half].reshape(C * R, CW)
        part = jnp.dot(x, wts[k * CW:(k + 1) * CW, :], preferred_element_type=F32)
        part = part.reshape(C, R, NW)
        if k > 0:
            part = part + acc[half]
        acc[half] = part
        if k == K - 1:
            tb[half] = part.astype(BF16)
            for o in range(1, H):
                zz = lax.rem(z + o, H)
                remote(
                    tb.at[half, pl.ds(zz * CZ, CZ)], tl.at[half, z],
                    z_send.at[phase], z_recv.at[phase], "head", zz,
                )

    def near(k):
        spread(k)
        if k == 0:
            wait(wts, load_sem.at[2])
        product(k, core, 0)

    def far(k):
        wait(qg.at[k, 1 - core], b_recv.at[k])
        product(k, 1 - core, 1)

    def key_value(k):
        g = group_of(k)
        fresh = (k * CH) % GROUP == 0
        last = ((k + 1) * CH) % GROUP == 0
        if fresh:
            kacc[...] = jnp.zeros_like(kacc)
            vacc[...] = jnp.zeros_like(vacc)

        def head(hh, carry):
            w, ds = weights_of(k, hh)
            kacc[...] += jnp.dot(ds, heads_of(k, 0, hh), preferred_element_type=F32)
            vacc[...] += jnp.dot(w.astype(BF16), heads_of(k, 1, hh), preferred_element_type=F32)
            return carry

        lax.fori_loop(0, CH, head, 0, unroll=True)
        if last:
            feats = slice(g * HEAD_DIM, (g + 1) * HEAD_DIM)
            kg_out[:, feats] = (kacc[...] * SCALE).astype(BF16)
            vg_out[:, feats] = vacc[...].astype(BF16)

    filled = 0

    def fill(upto):
        nonlocal filled
        for k in range(filled, min(upto, K)):
            key_value(k)
        filled = max(filled, min(upto, K))

    stages = (arrive, forward, backward, pair_sum, total_sum, near, far)
    for t in range(K + LAGS[-1]):
        for stage, lag in zip(stages, (0,) + LAGS):
            k = t - lag
            if 0 <= k < K:
                stage(k)
                if k == K - 1 and stage is pair_sum:
                    fill(K // 2)
                if k == K - 1 and stage is total_sum:
                    fill(3 * K // 4)
    fill(K)
    wait(tl.at[core, pl.ds(0, H - 1)], z_recv.at[0])
    wait(tl.at[1 - core, pl.ds(0, H - 1)], z_recv.at[1])
    for i in range(CZ):
        for half in range(2):
            s = acc[half, z * CZ + i]
            for o in range(1, H):
                s = s + tl[half, lax.rem(z + o, H), i].astype(F32)
            tg_out[(i * 2 + half) * R:(i * 2 + half + 1) * R, :] = s.astype(BF16)

    for k in range(K):
        for a in range(2):
            wait(land.at[k, a, core, pl.ds(0, C - 1)], g_send.at[k, a])
            wait(land.at[k, a, core], f_send.at[k, a])
        wait(stats.at[k, pl.ds(0, V - 1)], st_send.at[k])
        wait(dqs.at[k], x_send.at[k])
        wait(rsl.at[k, pl.ds(0, C - 1)], r_send.at[k])
        wait(qg.at[k, core, pl.ds(0, C - 1)], a_send.at[k])
        wait(qg.at[k, core], b_send.at[k])
    for half in range(2):
        wait(tl.at[half, pl.ds(0, H - 1)], z_send.at[half])


def write(*refs):
    count = len(refs) // 2
    sems = refs[-1]
    copies = [
        pltpu.make_async_copy(refs[i], refs[count + i], sems.at[i]) for i in range(count)
    ]
    for copy in copies:
        copy.start()
    for copy in copies:
        copy.wait()


def shards(V, H, text_queries, visual_keys, visual_values, out_grad, query_frame, block_frame, q_weight):
    R, QW = text_queries.shape
    T, KW = visual_keys.shape
    C = V // 2
    NQ = V * R
    NW = q_weight.shape[1]
    HL = QW // HEAD_DIM
    G = KW // HEAD_DIM
    K = HL // CH
    CW = CH * HEAD_DIM
    CZ = C // H
    frames = query_frame.reshape(1, NQ)
    vmem = pltpu.VMEM
    dma = pltpu.SemaphoreType.DMA
    any_spec = pl.BlockSpec(memory_space=pl.ANY)
    shapes = ((R, QW), (T, KW), (T, KW), (NQ // H, NW))
    grads = pl.pallas_call(
        functools.partial(kernel, V, H),
        out_shape=tuple(vmem(shape, BF16) for shape in shapes),
        in_specs=[
            pl.BlockSpec(memory_space=pltpu.VMEM),
            pl.BlockSpec(memory_space=pltpu.SMEM),
        ] + [any_spec] * 5,
        out_specs=(pl.BlockSpec(memory_space=vmem),) * 4,
        scratch_shapes=[
            vmem((K, 2, 2, C, R, CW), BF16),
            vmem((T, KW), BF16),
            vmem((T, KW), BF16),
            vmem((G, HEAD_DIM, T), BF16),
            vmem((QW, NW), BF16),
            vmem((T // BLOCK, NQ), F32),
            vmem((HL, T, NQ), F32),
            vmem((HL, T, NQ), F32),
            vmem((K, CH, NQ), F32),
            vmem((K, V, 2 * CH, NQ), F32),
            vmem((K, 2 * CH, NQ), F32),
            vmem((K, 2, C, R, CW), F32),
            vmem((K, C, R, CW), F32),
            vmem((K, C, R, CW), F32),
            vmem((K, C, R, CW), BF16),
            vmem((K, C, R, CW), BF16),
            vmem((K, 2, C, R, CW), BF16),
            vmem((2, C, R, NW), F32),
            vmem((2, C, R, NW), BF16),
            vmem((2, H, CZ, R, NW), BF16),
            vmem((T, HEAD_DIM), F32),
            vmem((T, HEAD_DIM), F32),
            dma((3,)), dma((K, 2)),
            dma((K, 2)), dma((K, 2)), dma((K, 2)), dma((K, 2)),
            dma((K,)), dma((K,)), dma((K,)), dma((K,)), dma((K,)), dma((K,)),
            dma((K,)), dma((K,)), dma((K,)), dma((K,)), dma((2,)), dma((2,)),
        ],
        compiler_params=pltpu.CompilerParams(
            collective_id=0, has_side_effects=True, vmem_limit_bytes=62_000_000
        ),
    )(frames, block_frame, text_queries, out_grad, visual_keys, visual_values, q_weight)
    return pl.pallas_call(
        write,
        out_shape=tuple(jax.ShapeDtypeStruct(shape, BF16) for shape in shapes),
        in_specs=[pl.BlockSpec(memory_space=vmem)] * 4,
        out_specs=(any_spec,) * 4,
        scratch_shapes=[dma((4,))],
    )(*[pltpu.with_memory_space_constraint(grad, vmem) for grad in grads])


def solution(mesh):
    in_specs = (
        P("video", "head"),
        P("video", "head"),
        P("video", "head"),
        P("video", "head"),
        P(),
        P(),
        P("head", "video"),
    )
    out_specs = (P("video", "head"), P("video", "head"), P("video", "head"), P("head", "video"))
    body = functools.partial(shards, mesh.shape["video"], mesh.shape["head"])
    return jax.shard_map(body, mesh=mesh, in_specs=in_specs, out_specs=out_specs, check_vma=False)
```
